128 devices in a mesh: wide: 16 (over x_hi, y, core), narrow: 8 (over z, x_lo).
Axes of the slice: x: 4 (x_hi: 2, x_lo: 2; x = x_hi * 2 + x_lo), y: 4, z: 4, core: 2. Of those that a mesh axis runs over, the one named last changes fastest.
Arguments:
- image: bfloat16 [2, 256, 256, 256], P(None, 'wide', 'narrow'), may hold values from -6 to 6
- deapodization: float32 [3, 256], replicated, may hold values from 0.5 to 2
- offsets: int32 [128, 16], P(('wide', 'narrow')), may hold values from 0 to 256
- cross_weight: bfloat16 [128, 16, 1536, 256], P(('wide', 'narrow')), may hold values from -0.375 to 0.375
- x_weight: bfloat16 [128, 16, 1536, 256], P(('wide', 'narrow')), may hold values from -0.375 to 0.375
Outputs:
- samples: float32 [128, 16, 2, 1536], P(('wide', 'narrow'))
The draws below stay inside these ranges and needn't reach their ends.
Inputs may be any that keep to these rules, and one draw needn't show every extreme that they name: `offsets`: each entry is the first row, along the first frequency dimension, of a group's window of 256 rows in one slab.
All inputs are finite; a program needn't handle non-finite values.
Results may differ from the reference program's by a relative error of at most 0.007.
Values may be sent and summed in bfloat16 or wider, within the bound.
A program may use at most 128 MiB of HBM per device.

```python
import math
import jax
import jax.numpy as jnp
from jax import lax

N = 256
G = 512
KZ = 64
BX = 256
SAMP = 1536
CROSS = 256
GROUPS = 128
N_WIDE = 16
N_NARROW = 8


def plant(array, stream_key, least, high):
    place = [jax.random.randint(jax.random.fold_in(stream_key, axis), (), 0, length) for axis, length in enumerate(array.shape)]
    longest = array.shape.index(max(array.shape))
    beside = place[:longest] + [(place[longest] + 1) % array.shape[longest]] + place[longest + 1:]
    return array.at[tuple(place)].set(least).at[tuple(beside)].set(high)


def steps_of(key, shape, cuts, least, high):
    level = 1.0
    for axis_at, shards_of in cuts:
        heights = jax.random.uniform(jax.random.fold_in(jax.random.fold_in(key, 6), axis_at), (shards_of,), jnp.float32, least / len(cuts), high / len(cuts))
        level = level * jnp.repeat(jnp.exp(heights), shape[axis_at] // shards_of).reshape((-1,) + (1,) * (len(shape) - 1 - axis_at))
    return level


def normal_values(key, dims, width, most, split=(), held_as=jnp.bfloat16):
    result = jax.random.normal(key, dims, jnp.float32) * width
    if len(split) > 0:
        result = steps_of(key, dims, split, -0.22, 0.18) * result
    return jnp.clip(result, min=-most, max=most).astype(held_as)


def setup_inputs(seed: int = 0) -> dict:
    arg_keys = jax.random.split(jax.random.key(seed), 6)
    return {
        "image": normal_values(arg_keys[0], (2, N, N, N), 1.0, 6.0, ((1, 16), (2, 8))),
        "deapodization": jnp.clip(jnp.exp(jax.random.uniform(arg_keys[1], (3, N), jnp.float32, math.log(0.5), math.log(2.0))), 0.5, 2.0),
        "offsets": plant(jax.random.randint(arg_keys[2], (GROUPS, N_WIDE), 0, G - BX + 1), jax.random.fold_in(arg_keys[2], 1), 0, G - BX).astype(jnp.int32),
        "cross_weight": normal_values(arg_keys[3], (GROUPS, N_WIDE, SAMP, CROSS), CROSS ** -0.5, 0.375, ((0, 128),)),
        "x_weight": normal_values(arg_keys[4], (GROUPS, N_WIDE, SAMP, BX), BX ** -0.5, 0.375, ((0, 128),)),
    }


def dft_tables(out_rows, inputs, grid_size, lowest):
    frequency = jnp.arange(out_rows, dtype=jnp.int32) + lowest
    position = jnp.arange(inputs, dtype=jnp.int32) - inputs // 2
    phases = jnp.mod(frequency[:, None] * position[None, :], grid_size)
    angles = phases.astype(jnp.float32) * (2.0 * math.pi / grid_size)
    factor = 1.0 / math.sqrt(inputs)
    return jnp.stack([jnp.cos(angles) * factor, jnp.sin(angles) * factor]).astype(jnp.bfloat16)

def mix_parts(product):
    return (product[0, 0] + product[1, 1], product[0, 1] - product[1, 0])

def reference(image, deapodization, offsets, cross_weight, x_weight):
    weighted = (image.astype(jnp.float32) * deapodization[0][None, :, None, None] * deapodization[1][None, None, :, None] * deapodization[2][None, None, None, :]).astype(jnp.bfloat16)
    z_table = dft_tables(KZ, N, G, -(KZ // 2)).astype(jnp.float32)
    product = jnp.einsum('tkz,cxyz->tcxyk', z_table, weighted.astype(jnp.float32))
    real_part, imag_part = mix_parts(product)
    band_data = jnp.stack([real_part, imag_part], axis=0).astype(jnp.bfloat16)
    line_table = dft_tables(G, N, G, -(G // 2)).astype(jnp.float32)
    product = jnp.einsum('tqy,cxyk->tcxqk', line_table, band_data.astype(jnp.float32))
    real_part, imag_part = mix_parts(product)
    columns = jnp.stack([real_part, imag_part], axis=0).astype(jnp.bfloat16)
    product = jnp.einsum('tpx,cxqk->tcpqk', line_table, columns.astype(jnp.float32))
    real_part, imag_part = mix_parts(product)
    kspace = jnp.stack([real_part, imag_part], axis=1).astype(jnp.bfloat16)
    span_y = G // N_WIDE
    span_z = KZ // N_NARROW

    def group_samples(group_index):
        narrow_pos = group_index % N_NARROW

        def slab_samples(slab_index):
            start_row = offsets[group_index, slab_index]
            window_rows = lax.dynamic_slice(kspace, (start_row, jnp.int32(0), slab_index * span_y, narrow_pos * span_z), (BX, 2, span_y, span_z)).reshape(BX, 2, span_y * span_z)
            cross_rows = cross_weight[group_index, slab_index].astype(jnp.float32)
            partial_value = jnp.einsum('ms,qcs->cmq', cross_rows, window_rows.astype(jnp.float32))
            window_gain = x_weight[group_index, slab_index].astype(jnp.float32)
            return lax.optimization_barrier(jnp.sum(partial_value * window_gain[None], axis=-1))
        return lax.map(slab_samples, jnp.arange(N_WIDE, dtype=jnp.int32))
    return lax.map(group_samples, jnp.arange(N_WIDE * N_NARROW, dtype=jnp.int32))
```

```python
import functools
import math

import jax
import jax.numpy as jnp
import ml_dtypes
import numpy as np
from jax import lax
from jax.experimental import pallas as pl
from jax.experimental.pallas import tpu as pltpu
from jax.sharding import PartitionSpec as P

F32 = jnp.float32
BF16 = jnp.bfloat16
MESH = pl.DeviceIdType.MESH
NT = (((1,), (1,)), ((), ()))
NN = (((1,), (0,)), ((), ()))


def trig(frequency, position):
    phase = np.mod(frequency[:, None] * position[None, :], 512)
    angle = phase * (2.0 * math.pi / 512)
    scale = 1.0 / math.sqrt(256)
    return np.cos(angle) * scale, np.sin(angle) * scale


def tables():
    position = np.arange(256) - 128
    cosine, sine = trig(np.arange(64) - 32, position)
    tz = np.zeros((2, 256, 8, 2, 8), np.float32)
    cos_t = cosine.reshape(8, 8, 256).transpose(2, 1, 0)
    sin_t = sine.reshape(8, 8, 256).transpose(2, 1, 0)
    tz[0, :, :, 0], tz[1, :, :, 0] = cos_t, sin_t
    tz[0, :, :, 1], tz[1, :, :, 1] = -sin_t, cos_t
    tz = tz.reshape(2, 256, 128)
    cosine, sine = trig(np.arange(512) - 256, position)
    ty = np.stack([cosine, sine])
    tx = ty[:, :256].reshape(2, 256, 2, 4, 2, 16).transpose(0, 1, 4, 2, 3, 5).reshape(2, 256, 256)
    return tz.astype(ml_dtypes.bfloat16), ty.astype(ml_dtypes.bfloat16), tx.astype(np.float32)


def kernel(
    img_h, deap, deap_s, off_s, cw_h, xw_h, tz_h, ty_h, tx_h, out,
    img, tz, ty, tx, dyz, send, blk, band, tyf, twin, col, cw, xw, xwt, win_a, win_b,
    in_sem, cw_sem, xw_sem, s1, r1, s2, r2, s3, r3,
):
    wide = lax.axis_index("wide")
    narrow = lax.axis_index("narrow")
    xh = wide // 8
    y = (wide // 2) % 4
    core = wide % 2
    me = xh * 8 + narrow

    def at_y(step):
        return {"wide": xh * 8 + ((y + step) % 4) * 2 + core, "narrow": narrow}

    other = {"wide": xh * 8 + y * 2 + (1 - core), "narrow": narrow}

    def peer(d):
        return {"wide": (d // 8) * 8 + y * 2 + core, "narrow": d % 8}

    ins = [
        pltpu.make_async_copy(img_h, img, in_sem.at[0]),
        pltpu.make_async_copy(tz_h, tz, in_sem.at[1]),
        pltpu.make_async_copy(ty_h, ty, in_sem.at[2]),
        pltpu.make_async_copy(tx_h, tx, in_sem.at[3]),
    ]
    for copy in ins:
        copy.start()

    def xw_copy(s):
        return pltpu.make_async_copy(xw_h.at[s], xw.at[s], xw_sem.at[s])

    def cw_copy(s):
        return pltpu.make_async_copy(cw_h.at[s], cw.at[s], cw_sem.at[s])

    barrier = pltpu.get_barrier_semaphore()

    def greet(i, _):
        pl.semaphore_signal(barrier, inc=1, device_id=peer((me + i) % 16), device_id_type=MESH)
        return 0

    lax.fori_loop(1, 16, greet, 0)
    for target in (at_y(1), at_y(3), other):
        pl.semaphore_signal(barrier, inc=1, device_id=target, device_id_type=MESH)

    dz = deap[2:3, :]
    for i in range(32):
        dyz[i : i + 1, :] = dz * deap_s[1, narrow * 32 + i]
    ins[0].wait()
    for x in range(16):
        gain = dyz[...] * deap_s[0, wide * 16 + x]
        for c in range(2):
            img[c, x] = (img[c, x].astype(F32) * gain).astype(BF16)
    ins[1].wait()
    freq = lax.dot_general(img[0].reshape(512, 256), tz[0], NN, preferred_element_type=F32)
    freq += lax.dot_general(img[1].reshape(512, 256), tz[1], NN, preferred_element_type=F32)
    lane = lax.broadcasted_iota(jnp.int32, (32, 128), 1)
    parts = [freq[x * 32 : (x + 1) * 32] for x in range(16)]
    for b in range(4):
        step = 1 << b
        low = (lane & step) == 0
        for x in range(16):
            if x & step:
                continue
            a0, a1 = parts[x], parts[x + step]
            parts[x] = jnp.where(low, a0, pltpu.roll(a1, step, 1))
            parts[x + step] = jnp.where(low, pltpu.roll(a0, 128 - step, 1), a1)
    for n in range(8):
        for c in range(2):
            send[n, c] = parts[c * 8 + n].astype(BF16)

    def start_xw(s, _):
        xw_copy(s).start()
        return 0

    def start_cw(s, _):
        cw_copy(s).start()
        return 0

    lax.fori_loop(0, 16, start_xw, 0)
    lax.fori_loop(0, 16, start_cw, 0)

    pl.semaphore_wait(barrier, 18)

    def piece(d, src):
        return pltpu.make_async_remote_copy(
            src_ref=send.at[d % 8],
            dst_ref=blk.at[src // 8, :, pl.ds(pl.multiple_of((src % 8) * 32, 32), 32), :],
            send_sem=s1.at[d],
            recv_sem=r1.at[src],
            device_id=peer(d),
            device_id_type=MESH,
        )

    def send_piece(i, _):
        piece((me + i) % 16, me).start()
        return 0

    lax.fori_loop(1, 16, send_piece, 0)
    blk[xh, :, pl.ds(pl.multiple_of(narrow * 32, 32), 32), :] = send[narrow]

    ins[2].wait()
    tyf[0, :, 0:256] = ty[0]
    tyf[0, :, 256:512] = ty[1]
    tyf[1, :, 0:256] = -ty[1]
    tyf[1, :, 256:512] = ty[0]
    ins[3].wait()

    place = lax.broadcasted_iota(jnp.int32, (8, 256), 1)
    place = (
        ((place >> 6) & 1) * 128 + ((place >> 4) & 3) * 32 + (place >> 7) * 16 + (place & 15) - 128
    )

    def windows(s, _):
        phase = (place * off_s[0, s]) & 511
        angle = phase.astype(F32) * (2.0 * math.pi / 512)
        cosine, sine = jnp.cos(angle)[0:1], jnp.sin(angle)[0:1]
        twin[s, 0] = (tx[0] * cosine - tx[1] * sine).astype(BF16)
        twin[s, 1] = (tx[1] * cosine + tx[0] * sine).astype(BF16)
        return 0

    lax.fori_loop(0, 16, windows, 0)

    def transpose_slabs(first, last):
        def one(s, _):
            xw_copy(s).wait()
            for j in range(6):
                xwt[s, j] = xw[s, j * 256 : (j + 1) * 256, :].T
            return 0

        lax.fori_loop(first, last, one, 0)

    def got_piece(i, _):
        piece(me, (me + i) % 16).wait_recv()
        return 0

    lax.fori_loop(1, 16, got_piece, 0)

    b0, b1 = blk[0].reshape(512, 128), blk[1].reshape(512, 128)
    band[0, y, core] = jnp.concatenate([b0[:, :64], b1[:, :64]], axis=1)
    band[1, y, core] = jnp.concatenate([b0[:, 64:], b1[:, 64:]], axis=1)

    def ring(kg, kind, slot, step):
        return pltpu.make_async_remote_copy(
            src_ref=band.at[kg, (y + slot) % 4, core],
            dst_ref=band.at[kg, (y + slot) % 4, core],
            send_sem=s2.at[kg, kind],
            recv_sem=r2.at[kg, kind],
            device_id=at_y(step),
            device_id_type=MESH,
        )

    def got_ring(kg, kind, slot):
        return pltpu.make_async_remote_copy(
            src_ref=band.at[kg, (y + slot) % 4, core],
            dst_ref=band.at[kg, (y + slot) % 4, core],
            send_sem=s2.at[kg, kind],
            recv_sem=r2.at[kg, kind],
            device_id=at_y(1),
            device_id_type=MESH,
        )

    def across(kg, slot, side):
        return pltpu.make_async_remote_copy(
            src_ref=band.at[kg, (y + slot) % 4, side],
            dst_ref=band.at[kg, (y + slot) % 4, side],
            send_sem=s3.at[kg, slot],
            recv_sem=r3.at[kg, slot],
            device_id=other,
            device_id_type=MESH,
        )

    ring(0, 0, 0, 1).start()
    ring(0, 1, 0, 3).start()
    ring(1, 1, 0, 3).start()
    across(0, 0, core).start()
    across(1, 0, core).start()

    transpose_slabs(0, 5)

    got_ring(0, 0, 3).wait_recv()
    ring(0, 2, 3, 1).start()
    ring(1, 0, 0, 1).start()
    across(0, 3, core).start()
    got_ring(0, 1, 1).wait_recv()
    across(0, 1, core).start()

    transpose_slabs(5, 11)

    got_ring(1, 1, 1).wait_recv()
    ring(1, 2, 1, 3).start()
    across(1, 1, core).start()
    got_ring(0, 2, 2).wait_recv()
    across(0, 2, core).start()

    transpose_slabs(11, 16)

    got_ring(1, 0, 3).wait_recv()
    across(1, 3, core).start()

    def lines(kg):
        lane_b = lax.broadcasted_iota(jnp.int32, (512, 128), 1)
        sides = []
        for side in range(2):
            rows = [band[kg, i, side].astype(F32) for i in range(4)]
            for b in range(2):
                step, shift = 1 << b, 16 << b
                low = (lane_b & shift) == 0
                for i in range(4):
                    if i & step:
                        continue
                    a0, a1 = rows[i], rows[i + step]
                    rows[i] = jnp.where(low, a0, pltpu.roll(a1, shift, 1))
                    rows[i + step] = jnp.where(low, pltpu.roll(a0, 128 - shift, 1), a1)
            sides.append([r.astype(BF16) for r in rows])
        for k in range(4):
            data = jnp.concatenate([sides[0][k], sides[1][k]], axis=1)
            for c in range(2):
                line = lax.dot_general(tyf[c], data, NN, preferred_element_type=F32)
                for s in range(16):
                    for t in range(2):
                        col[s, c, t, pl.ds(kg * 4 + k, 32, stride=8), :] = line[
                            s * 32 : (s + 1) * 32, t * 128 : (t + 1) * 128
                        ]

    for slot in range(4):
        across(0, slot, 1 - core).wait_recv()
    lines(0)
    got_ring(1, 2, 2).wait_recv()
    across(1, 2, core).start()
    for slot in range(4):
        across(1, slot, 1 - core).wait_recv()
    lines(1)

    def got_cw(s, _):
        cw_copy(s).wait()
        return 0

    lax.fori_loop(0, 16, got_cw, 0)

    def to_window(s, win):
        cosine, sine = twin[s, 0], twin[s, 1]
        real = jnp.concatenate([cosine, sine], axis=1)
        imag = jnp.concatenate([-sine, cosine], axis=1)
        source = jnp.concatenate(
            [col[s, c, t].astype(BF16) for c in range(2) for t in range(2)], axis=1
        )
        win[0:256] = lax.dot_general(real, source, NT, preferred_element_type=F32).astype(BF16)
        win[256:512] = lax.dot_general(imag, source, NT, preferred_element_type=F32).astype(BF16)

    def to_samples(s, win):
        for j in range(6):
            rows = cw[s, j * 256 : (j + 1) * 256, :]
            part = lax.dot_general(win[...], rows, NT, preferred_element_type=F32)
            gain = xwt[s, j].astype(F32)
            here = slice(j * 256, (j + 1) * 256)
            out[s, 0:1, here] = jnp.sum(part[:256] * gain, axis=0, keepdims=True)
            out[s, 1:2, here] = jnp.sum(part[256:] * gain, axis=0, keepdims=True)

    to_window(0, win_a)

    def pair(i, _):
        s = i * 2
        to_window(s + 1, win_b)
        to_samples(s, win_a)
        to_window((s + 2) % 16, win_a)
        to_samples(s + 1, win_b)
        return 0

    lax.fori_loop(0, 8, pair, 0)

    def sent(i, _):
        piece((me + i) % 16, me).wait_send()
        return 0

    lax.fori_loop(1, 16, sent, 0)
    for kg in range(2):
        ring(kg, 0, 0, 1).wait_send()
        ring(kg, 1, 0, 3).wait_send()
        for slot in range(4):
            across(kg, slot, core).wait_send()
    ring(0, 2, 3, 1).wait_send()
    ring(1, 2, 1, 3).wait_send()


def per_device(image, deapodization, offsets, cross_weight, x_weight):
    tz, ty, tx = (jnp.asarray(t) for t in tables())
    any_space = pl.BlockSpec(memory_space=pl.ANY)
    smem = pl.BlockSpec(memory_space=pltpu.SMEM)
    vmem = pl.BlockSpec(memory_space=pltpu.VMEM)
    dma = pltpu.SemaphoreType.DMA
    samples = pl.pallas_call(
        kernel,
        out_shape=jax.ShapeDtypeStruct((16, 2, 1536), F32),
        in_specs=[any_space, vmem, smem, smem] + [any_space] * 5,
        out_specs=vmem,
        scratch_shapes=[
            pltpu.VMEM((2, 16, 32, 256), BF16),
            pltpu.VMEM((2, 256, 128), BF16),
            pltpu.VMEM((2, 512, 256), BF16),
            pltpu.VMEM((2, 256, 256), F32),
            pltpu.VMEM((32, 256), F32),
            pltpu.VMEM((8, 2, 32, 128), BF16),
            pltpu.VMEM((2, 2, 256, 128), BF16),
            pltpu.VMEM((2, 4, 2, 512, 128), BF16),
            pltpu.VMEM((2, 512, 512), BF16),
            pltpu.VMEM((16, 2, 256, 256), BF16),
            pltpu.VMEM((16, 2, 2, 256, 128), F32),
            pltpu.VMEM((16, 1536, 256), BF16),
            pltpu.VMEM((16, 1536, 256), BF16),
            pltpu.VMEM((16, 6, 256, 256), BF16),
            pltpu.VMEM((512, 256), BF16),
            pltpu.VMEM((512, 256), BF16),
            dma((4,)),
            dma((16,)),
            dma((16,)),
            dma((16,)),
            dma((16,)),
            dma((2, 3)),
            dma((2, 3)),
            dma((2, 4)),
            dma((2, 4)),
        ],
        compiler_params=pltpu.CompilerParams(
            collective_id=0, has_side_effects=True, vmem_limit_bytes=67043328
        ),
        cost_estimate=pl.CostEstimate(flops=11_000_000_000, bytes_accessed=28_000_000, transcendentals=0),
        name="spokes",
    )(image, deapodization, deapodization, offsets, cross_weight[0], x_weight[0], tz, ty, tx)
    return samples[None]


def solution(mesh):
    return jax.shard_map(
        per_device,
        mesh=mesh,
        in_specs=(
            P(None, "wide", "narrow", None),
            P(),
            P(("wide", "narrow"), None),
            P(("wide", "narrow"), None, None, None),
            P(("wide", "narrow"), None, None, None),
        ),
        out_specs=P(("wide", "narrow"), None, None, None),
        check_vma=False,
    )
```

```python
import functools
import math

import jax
import jax.numpy as jnp
import ml_dtypes
import numpy as np
from jax import lax
from jax.experimental import pallas as pl
from jax.experimental.pallas import tpu as pltpu
from jax.sharding import PartitionSpec as P

F32 = jnp.float32
BF16 = jnp.bfloat16
MESH = pl.DeviceIdType.MESH
NT = (((1,), (1,)), ((), ()))
NN = (((1,), (0,)), ((), ()))


def trig(frequency, position):
    phase = np.mod(frequency[:, None] * position[None, :], 512)
    angle = phase * (2.0 * math.pi / 512)
    scale = 1.0 / math.sqrt(256)
    return np.cos(angle) * scale, np.sin(angle) * scale


def tables():
    position = np.arange(256) - 128
    cosine, sine = trig(np.arange(64) - 32, position)
    tz = np.zeros((2, 256, 8, 2, 8), np.float32)
    cos_t = cosine.reshape(8, 8, 256).transpose(2, 1, 0)
    sin_t = sine.reshape(8, 8, 256).transpose(2, 1, 0)
    tz[0, :, :, 0], tz[1, :, :, 0] = cos_t, sin_t
    tz[0, :, :, 1], tz[1, :, :, 1] = -sin_t, cos_t
    tz = tz.reshape(2, 256, 128)
    cosine, sine = trig(np.arange(512) - 256, position)
    ty = np.stack([cosine, sine])
    tx = ty[:, :256].reshape(2, 256, 2, 4, 2, 16).transpose(0, 1, 4, 2, 3, 5).reshape(2, 256, 256)
    return tz.astype(ml_dtypes.bfloat16), ty.astype(ml_dtypes.bfloat16), tx.astype(np.float32)


def kernel(
    img_h, deap, deap_s, off_s, cw_h, xw_h, tz_h, ty_h, tx_h, out,
    img, tz, ty, tx, dyz, send, blk, band, tyf, twin, col, cw, xw, xwt, win_a, win_b,
    in_sem, cw_sem, xw_sem, s1, r1, s2, r2, s3, r3,
):
    wide = lax.axis_index("wide")
    narrow = lax.axis_index("narrow")
    xh = wide // 8
    y = (wide // 2) % 4
    core = wide % 2
    me = xh * 8 + narrow

    def at_y(step):
        return {"wide": xh * 8 + ((y + step) % 4) * 2 + core, "narrow": narrow}

    other = {"wide": xh * 8 + y * 2 + (1 - core), "narrow": narrow}

    def peer(d):
        return {"wide": (d // 8) * 8 + y * 2 + core, "narrow": d % 8}

    ins = [
        pltpu.make_async_copy(img_h, img, in_sem.at[0]),
        pltpu.make_async_copy(tz_h, tz, in_sem.at[1]),
        pltpu.make_async_copy(ty_h, ty, in_sem.at[2]),
        pltpu.make_async_copy(tx_h, tx, in_sem.at[3]),
    ]
    for copy in ins:
        copy.start()

    def xw_copy(s):
        return pltpu.make_async_copy(xw_h.at[s], xw.at[s], xw_sem.at[s])

    def cw_copy(s):
        return pltpu.make_async_copy(cw_h.at[s], cw.at[s], cw_sem.at[s])

    barrier = pltpu.get_barrier_semaphore()

    def greet(i, _):
        pl.semaphore_signal(barrier, inc=1, device_id=peer((me + i) % 16), device_id_type=MESH)
        return 0

    lax.fori_loop(1, 16, greet, 0)
    for target in (at_y(1), at_y(3), other):
        pl.semaphore_signal(barrier, inc=1, device_id=target, device_id_type=MESH)

    dz = deap[2:3, :]
    for i in range(32):
        dyz[i : i + 1, :] = dz * deap_s[1, narrow * 32 + i]
    ins[0].wait()
    for x in range(16):
        gain = dyz[...] * deap_s[0, wide * 16 + x]
        for c in range(2):
            img[c, x] = (img[c, x].astype(F32) * gain).astype(BF16)
    ins[1].wait()
    freq = lax.dot_general(img[0].reshape(512, 256), tz[0], NN, preferred_element_type=F32)
    freq += lax.dot_general(img[1].reshape(512, 256), tz[1], NN, preferred_element_type=F32)
    lane = lax.broadcasted_iota(jnp.int32, (32, 128), 1)
    parts = [freq[x * 32 : (x + 1) * 32] for x in range(16)]
    for b in range(4):
        step = 1 << b
        low = (lane & step) == 0
        for x in range(16):
            if x & step:
                continue
            a0, a1 = parts[x], parts[x + step]
            parts[x] = jnp.where(low, a0, pltpu.roll(a1, step, 1))
            parts[x + step] = jnp.where(low, pltpu.roll(a0, 128 - step, 1), a1)
    for n in range(8):
        for c in range(2):
            send[n, c] = parts[c * 8 + n].astype(BF16)

    def start_xw(s, _):
        xw_copy(s).start()
        return 0

    def start_cw(s, _):
        cw_copy(s).start()
        return 0

    lax.fori_loop(0, 16, start_xw, 0)
    lax.fori_loop(0, 16, start_cw, 0)

    ins[2].wait()
    tyf[0, :, 0:256] = ty[0]
    tyf[0, :, 256:512] = ty[1]
    tyf[1, :, 0:256] = -ty[1]
    tyf[1, :, 256:512] = ty[0]
    ins[3].wait()

    place = lax.broadcasted_iota(jnp.int32, (8, 256), 1)
    place = (
        ((place >> 6) & 1) * 128 + ((place >> 4) & 3) * 32 + (place >> 7) * 16 + (place & 15) - 128
    )

    def windows(s, _):
        phase = (place * off_s[0, s]) & 511
        angle = phase.astype(F32) * (2.0 * math.pi / 512)
        cosine, sine = jnp.cos(angle)[0:1], jnp.sin(angle)[0:1]
        twin[s, 0] = (tx[0] * cosine - tx[1] * sine).astype(BF16)
        twin[s, 1] = (tx[1] * cosine + tx[0] * sine).astype(BF16)
        return 0

    lax.fori_loop(0, 16, windows, 0)

    pl.semaphore_wait(barrier, 18)

    def piece(d, src):
        return pltpu.make_async_remote_copy(
            src_ref=send.at[d % 8],
            dst_ref=blk.at[src // 8, :, pl.ds(pl.multiple_of((src % 8) * 32, 32), 32), :],
            send_sem=s1.at[d],
            recv_sem=r1.at[src],
            device_id=peer(d),
            device_id_type=MESH,
        )

    def send_piece(i, _):
        piece((me + i) % 16, me).start()
        return 0

    lax.fori_loop(1, 16, send_piece, 0)
    blk[xh, :, pl.ds(pl.multiple_of(narrow * 32, 32), 32), :] = send[narrow]

    def transpose_slabs(first, last):
        def one(s, _):
            xw_copy(s).wait()
            for j in range(6):
                xwt[s, j] = xw[s, j * 256 : (j + 1) * 256, :].T
            return 0

        lax.fori_loop(first, last, one, 0)

    transpose_slabs(0, 7)

    def got_piece(i, _):
        piece(me, (me + i) % 16).wait_recv()
        return 0

    lax.fori_loop(1, 16, got_piece, 0)

    b0, b1 = blk[0].reshape(512, 128), blk[1].reshape(512, 128)
    band[0, y, core] = jnp.concatenate([b0[:, :64], b1[:, :64]], axis=1)
    band[1, y, core] = jnp.concatenate([b0[:, 64:], b1[:, 64:]], axis=1)

    def ring(chunk, kind, slot, step):
        part = band.at[chunk // 2, (y + slot) % 4, core, pl.ds((chunk % 2) * 256, 256), :]
        return pltpu.make_async_remote_copy(
            src_ref=part,
            dst_ref=part,
            send_sem=s2.at[chunk, kind],
            recv_sem=r2.at[chunk, kind],
            device_id=at_y(step),
            device_id_type=MESH,
        )

    def across(chunk, slot, side):
        part = band.at[chunk // 2, (y + slot) % 4, side, pl.ds((chunk % 2) * 256, 256), :]
        return pltpu.make_async_remote_copy(
            src_ref=part,
            dst_ref=part,
            send_sem=s3.at[chunk, slot],
            recv_sem=r3.at[chunk, slot],
            device_id=other,
            device_id_type=MESH,
        )

    def from_below(chunk):
        ring(chunk, 0, 3, 1).wait_recv()
        if chunk < 2:
            ring(chunk, 2, 3, 1).start()
        across(chunk, 3, core).start()

    def from_above(chunk):
        ring(chunk, 1, 1, 3).wait_recv()
        if chunk >= 2:
            ring(chunk, 2, 1, 3).start()
        across(chunk, 1, core).start()

    def from_far(chunk):
        ring(chunk, 2, 2, 1).wait_recv()
        across(chunk, 2, core).start()

    for up, down in ((0, 2), (1, 3), (2, 0)):
        ring(up, 0, 0, 1).start()
        ring(down, 1, 0, 3).start()
    ring(1, 1, 0, 3).start()
    for chunk in range(4):
        across(chunk, 0, core).start()

    transpose_slabs(7, 12)
    from_below(0)
    from_above(2)
    transpose_slabs(12, 14)
    from_below(1)
    ring(3, 0, 0, 1).start()
    from_above(3)
    transpose_slabs(14, 15)
    from_below(2)
    from_above(0)
    transpose_slabs(15, 16)
    from_above(1)
    from_far(0)
    from_far(1)
    from_far(2)

    def lines(kg):
        lane_b = lax.broadcasted_iota(jnp.int32, (512, 128), 1)
        sides = []
        for side in range(2):
            rows = [band[kg, i, side].astype(F32) for i in range(4)]
            for b in range(2):
                step, shift = 1 << b, 16 << b
                low = (lane_b & shift) == 0
                for i in range(4):
                    if i & step:
                        continue
                    a0, a1 = rows[i], rows[i + step]
                    rows[i] = jnp.where(low, a0, pltpu.roll(a1, shift, 1))
                    rows[i + step] = jnp.where(low, pltpu.roll(a0, 128 - shift, 1), a1)
            sides.append([r.astype(BF16) for r in rows])
        for k in range(4):
            data = jnp.concatenate([sides[0][k], sides[1][k]], axis=1)
            for c in range(2):
                line = lax.dot_general(tyf[c], data, NN, preferred_element_type=F32)
                for s in range(16):
                    for t in range(2):
                        col[s, c, t, pl.ds(kg * 4 + k, 32, stride=8), :] = line[
                            s * 32 : (s + 1) * 32, t * 128 : (t + 1) * 128
                        ]

    for chunk in range(2):
        for slot in range(4):
            across(chunk, slot, 1 - core).wait_recv()
    lines(0)
    from_below(3)
    from_far(3)
    for chunk in range(2, 4):
        for slot in range(4):
            across(chunk, slot, 1 - core).wait_recv()
    lines(1)

    def got_cw(s, _):
        cw_copy(s).wait()
        return 0

    lax.fori_loop(0, 16, got_cw, 0)

    def to_window(s, win):
        cosine, sine = twin[s, 0], twin[s, 1]
        real = jnp.concatenate([cosine, sine], axis=1)
        imag = jnp.concatenate([-sine, cosine], axis=1)
        source = jnp.concatenate(
            [col[s, c, t].astype(BF16) for c in range(2) for t in range(2)], axis=1
        )
        win[0:256] = lax.dot_general(real, source, NT, preferred_element_type=F32).astype(BF16)
        win[256:512] = lax.dot_general(imag, source, NT, preferred_element_type=F32).astype(BF16)

    def to_samples(s, win):
        for j in range(6):
            rows = cw[s, j * 256 : (j + 1) * 256, :]
            part = lax.dot_general(win[...], rows, NT, preferred_element_type=F32)
            gain = xwt[s, j].astype(F32)
            here = slice(j * 256, (j + 1) * 256)
            out[s, 0:1, here] = jnp.sum(part[:256] * gain, axis=0, keepdims=True)
            out[s, 1:2, here] = jnp.sum(part[256:] * gain, axis=0, keepdims=True)

    to_window(0, win_a)
    wins = (win_a, win_b)

    def group(i, _):
        for u in range(8):
            s = i * 8 + u
            to_window((s + 1) % 16, wins[(u + 1) % 2])
            to_samples(s, wins[u % 2])
        return 0

    lax.fori_loop(0, 2, group, 0)

    def sent(i, _):
        piece((me + i) % 16, me).wait_send()
        return 0

    lax.fori_loop(1, 16, sent, 0)
    for chunk in range(4):
        ring(chunk, 0, 0, 1).wait_send()
        ring(chunk, 1, 0, 3).wait_send()
        ring(chunk, 2, 3, 1).wait_send()
        for slot in range(4):
            across(chunk, slot, core).wait_send()


def per_device(image, deapodization, offsets, cross_weight, x_weight):
    tz, ty, tx = (jnp.asarray(t) for t in tables())
    any_space = pl.BlockSpec(memory_space=pl.ANY)
    smem = pl.BlockSpec(memory_space=pltpu.SMEM)
    vmem = pl.BlockSpec(memory_space=pltpu.VMEM)
    dma = pltpu.SemaphoreType.DMA
    samples = pl.pallas_call(
        kernel,
        out_shape=jax.ShapeDtypeStruct((16, 2, 1536), F32),
        in_specs=[any_space, vmem, smem, smem] + [any_space] * 5,
        out_specs=vmem,
        scratch_shapes=[
            pltpu.VMEM((2, 16, 32, 256), BF16),
            pltpu.VMEM((2, 256, 128), BF16),
            pltpu.VMEM((2, 512, 256), BF16),
            pltpu.VMEM((2, 256, 256), F32),
            pltpu.VMEM((32, 256), F32),
            pltpu.VMEM((8, 2, 32, 128), BF16),
            pltpu.VMEM((2, 2, 256, 128), BF16),
            pltpu.VMEM((2, 4, 2, 512, 128), BF16),
            pltpu.VMEM((2, 512, 512), BF16),
            pltpu.VMEM((16, 2, 256, 256), BF16),
            pltpu.VMEM((16, 2, 2, 256, 128), F32),
            pltpu.VMEM((16, 1536, 256), BF16),
            pltpu.VMEM((16, 1536, 256), BF16),
            pltpu.VMEM((16, 6, 256, 256), BF16),
            pltpu.VMEM((512, 256), BF16),
            pltpu.VMEM((512, 256), BF16),
            dma((4,)),
            dma((16,)),
            dma((16,)),
            dma((16,)),
            dma((16,)),
            dma((4, 3)),
            dma((4, 3)),
            dma((4, 4)),
            dma((4, 4)),
        ],
        compiler_params=pltpu.CompilerParams(
            collective_id=0, has_side_effects=True, vmem_limit_bytes=67043328
        ),
        cost_estimate=pl.CostEstimate(flops=11_000_000_000, bytes_accessed=28_000_000, transcendentals=0),
        name="spokes",
    )(image, deapodization, deapodization, offsets, cross_weight[0], x_weight[0], tz, ty, tx)
    return samples[None]


def solution(mesh):
    return jax.shard_map(
        per_device,
        mesh=mesh,
        in_specs=(
            P(None, "wide", "narrow", None),
            P(),
            P(("wide", "narrow"), None),
            P(("wide", "narrow"), None, None, None),
            P(("wide", "narrow"), None, None, None),
        ),
        out_specs=P(("wide", "narrow"), None, None, None),
        check_vma=False,
    )
```

```python
import functools
import math

import jax
import jax.numpy as jnp
import ml_dtypes
import numpy as np
from jax import lax
from jax.experimental import pallas as pl
from jax.experimental.pallas import tpu as pltpu
from jax.sharding import PartitionSpec as P

F32 = jnp.float32
BF16 = jnp.bfloat16
MESH = pl.DeviceIdType.MESH
NT = (((1,), (1,)), ((), ()))
NN = (((1,), (0,)), ((), ()))


def trig(frequency, position):
    phase = np.mod(frequency[:, None] * position[None, :], 512)
    angle = phase * (2.0 * math.pi / 512)
    scale = 1.0 / math.sqrt(256)
    return np.cos(angle) * scale, np.sin(angle) * scale


def tables():
    position = np.arange(256) - 128
    cosine, sine = trig(np.arange(64) - 32, position)
    tz = np.zeros((2, 256, 8, 2, 8), np.float32)
    cos_t = cosine.reshape(8, 8, 256).transpose(2, 1, 0)
    sin_t = sine.reshape(8, 8, 256).transpose(2, 1, 0)
    tz[0, :, :, 0], tz[1, :, :, 0] = cos_t, sin_t
    tz[0, :, :, 1], tz[1, :, :, 1] = -sin_t, cos_t
    tz = tz.reshape(2, 256, 128)
    cosine, sine = trig(np.arange(512) - 256, position)
    ty = np.concatenate([cosine, sine], axis=1)
    tx = np.stack([cosine, sine])[:, :256].reshape(2, 256, 2, 4, 2, 16)
    tx = tx.transpose(0, 1, 3, 4, 2, 5).reshape(2, 256, 256)
    return tz.astype(ml_dtypes.bfloat16), ty.astype(ml_dtypes.bfloat16), tx.astype(np.float32)


def kernel(
    img_h, deap, deap_s, off_s, cw_h, xw_h, tz_h, ty_h, tx_h, out,
    img, tz, ty, tx, dyz, send, blk, band, mix, turn, twin, acc, col, cw, xw, xwt, win_a, win_b,
    in_sem, cw_sem, xw_sem, s1, r1, s2, r2, s3, r3,
):
    wide = lax.axis_index("wide")
    narrow = lax.axis_index("narrow")
    xh = wide // 8
    y = (wide // 2) % 4
    core = wide % 2
    me = xh * 8 + narrow

    def at_y(step):
        return {"wide": xh * 8 + ((y + step) % 4) * 2 + core, "narrow": narrow}

    other = {"wide": xh * 8 + y * 2 + (1 - core), "narrow": narrow}

    def peer(d):
        return {"wide": (d // 8) * 8 + y * 2 + core, "narrow": d % 8}

    ins = [
        pltpu.make_async_copy(img_h, img, in_sem.at[0]),
        pltpu.make_async_copy(tz_h, tz, in_sem.at[1]),
        pltpu.make_async_copy(ty_h, ty, in_sem.at[2]),
        pltpu.make_async_copy(tx_h, tx, in_sem.at[3]),
    ]
    for copy in ins:
        copy.start()

    def xw_copy(s):
        return pltpu.make_async_copy(xw_h.at[s], xw.at[s % 8], xw_sem.at[s])

    def cw_copy(s):
        return pltpu.make_async_copy(cw_h.at[s], cw.at[s], cw_sem.at[s])

    barrier = pltpu.get_barrier_semaphore()

    def greet(i, _):
        pl.semaphore_signal(barrier, inc=1, device_id=peer((me + i) % 16), device_id_type=MESH)
        return 0

    lax.fori_loop(1, 16, greet, 0)
    def diagonal(step):
        return {"wide": xh * 8 + ((y + step) % 4) * 2 + (1 - core), "narrow": narrow}

    for target in (at_y(1), at_y(3), other, diagonal(1), diagonal(3)):
        pl.semaphore_signal(barrier, inc=1, device_id=target, device_id_type=MESH)

    dz = deap[2:3, :]
    for i in range(32):
        dyz[i : i + 1, :] = dz * deap_s[1, narrow * 32 + i]
    ins[0].wait()
    for x in range(16):
        gain = dyz[...] * deap_s[0, wide * 16 + x]
        for c in range(2):
            img[c, x] = (img[c, x].astype(F32) * gain).astype(BF16)
    ins[1].wait()
    freq = lax.dot_general(img[0].reshape(512, 256), tz[0], NN, preferred_element_type=F32)
    freq += lax.dot_general(img[1].reshape(512, 256), tz[1], NN, preferred_element_type=F32)
    lane = lax.broadcasted_iota(jnp.int32, (32, 128), 1)
    parts = [freq[x * 32 : (x + 1) * 32] for x in range(16)]
    for b in range(4):
        step = 1 << b
        low = (lane & step) == 0
        for x in range(16):
            if x & step:
                continue
            a0, a1 = parts[x], parts[x + step]
            parts[x] = jnp.where(low, a0, pltpu.roll(a1, step, 1))
            parts[x + step] = jnp.where(low, pltpu.roll(a0, 128 - step, 1), a1)
    for n in range(8):
        for c in range(2):
            send[n, c] = parts[c * 8 + n].astype(BF16)

    def start_xw(s, _):
        xw_copy(s).start()
        return 0

    def start_cw(s, _):
        cw_copy(s).start()
        return 0

    lax.fori_loop(0, 8, start_xw, 0)
    lax.fori_loop(0, 16, start_cw, 0)

    row = lax.broadcasted_iota(jnp.int32, (512, 512), 0)
    goal = (
        ((row >> 4) & 3) * 128 + (row >> 8) * 64 + ((row >> 7) & 1) * 32 + ((row >> 6) & 1) * 16
    ) + (row & 15)
    mix[...] = (goal == lax.broadcasted_iota(jnp.int32, (512, 512), 1)).astype(BF16)

    ins[2].wait()
    ins[3].wait()
    low = lax.broadcasted_iota(jnp.int32, (256, 128), 1) < 64
    shift = ((4 - y) % 4) * 64
    cos_r, sin_r = pltpu.roll(tx[0], shift, 1), pltpu.roll(tx[1], shift, 1)
    c0, c1, z0, z1 = cos_r[:, :128], cos_r[:, 128:], sin_r[:, :128], sin_r[:, 128:]

    def swap(v):
        return pltpu.roll(v, 64, 1)

    turn[0, :, 0:128] = jnp.where(low, c0, swap(z0))
    turn[1, :, 0:128] = jnp.where(low, -z0, swap(c0))
    turn[0, :, 128:256] = jnp.where(low, swap(c0), z0)
    turn[1, :, 128:256] = jnp.where(low, -swap(z0), c0)
    turn[0, :, 256:384] = jnp.where(low, swap(c1), z1)
    turn[1, :, 256:384] = jnp.where(low, -swap(z1), c1)
    turn[0, :, 384:512] = jnp.where(low, c1, swap(z1))
    turn[1, :, 384:512] = jnp.where(low, -z1, swap(c1))

    place = lax.broadcasted_iota(jnp.int32, (8, 512), 1)
    tile = place >> 7
    away = jnp.where(tile < 2, tile, 5 - tile)
    place = (
        ((place >> 4) & 1) * 128 + ((y + away) & 3) * 32 + ((place >> 5) & 1) * 16 + (place & 15) - 128
    )

    def windows(s, _):
        phase = (place * off_s[0, s]) & 511
        angle = phase.astype(F32) * (2.0 * math.pi / 512)
        cosine, sine = jnp.cos(angle)[0:1], jnp.sin(angle)[0:1]
        twin[s] = (turn[0] * cosine + turn[1] * sine).astype(BF16)
        return 0

    def transpose_slabs(first, last):
        def one(s, _):
            xw_copy(s).wait()
            for j in range(6):
                xwt[s, j] = xw[s % 8, j * 256 : (j + 1) * 256, :].T
            return 0

        def one_and_next(s, _):
            one(s, 0)
            xw_copy(s + 8).start()
            return 0

        if first < 8:
            lax.fori_loop(first, min(last, 8), one_and_next, 0)
        if last > 8:
            lax.fori_loop(max(first, 8), last, one, 0)

    pl.semaphore_wait(barrier, 20)

    def piece(d, src):
        return pltpu.make_async_remote_copy(
            src_ref=send.at[d % 8],
            dst_ref=blk.at[src // 8, :, pl.ds(pl.multiple_of((src % 8) * 32, 32), 32), :],
            send_sem=s1.at[d],
            recv_sem=r1.at[src],
            device_id=peer(d),
            device_id_type=MESH,
        )

    def send_piece(i, _):
        piece((me + i) % 16, me).start()
        return 0

    lax.fori_loop(1, 16, send_piece, 0)
    blk[xh, :, pl.ds(pl.multiple_of(narrow * 32, 32), 32), :] = send[narrow]

    lax.fori_loop(0, 16, windows, 0)
    transpose_slabs(0, 6)

    def got_piece(i, _):
        piece(me, (me + i) % 16).wait_recv()
        return 0

    lax.fori_loop(1, 16, got_piece, 0)

    b0, b1 = blk[0].reshape(512, 128), blk[1].reshape(512, 128)
    band[0, y, core] = jnp.concatenate([b0[:, :64], b1[:, :64]], axis=1)
    band[1, y, core] = jnp.concatenate([b0[:, 64:], b1[:, 64:]], axis=1)

    def ring(chunk, kind, slot, step):
        part = band.at[chunk // 2, (y + slot) % 4, core, pl.ds((chunk % 2) * 256, 256), :]
        return pltpu.make_async_remote_copy(
            src_ref=part,
            dst_ref=part,
            send_sem=s2.at[chunk, kind],
            recv_sem=r2.at[chunk, kind],
            device_id=at_y(step),
            device_id_type=MESH,
        )

    def across(chunk, slot, side):
        part = band.at[chunk // 2, (y + slot) % 4, side, pl.ds((chunk % 2) * 256, 256), :]
        return pltpu.make_async_remote_copy(
            src_ref=part,
            dst_ref=part,
            send_sem=s3.at[chunk, slot],
            recv_sem=r3.at[chunk, slot],
            device_id=other,
            device_id_type=MESH,
        )

    def pass_on(chunk, slot, step):
        part = band.at[chunk // 2, (y + slot) % 4, core, pl.ds((chunk % 2) * 256, 256), :]
        return pltpu.make_async_remote_copy(
            src_ref=part,
            dst_ref=part,
            send_sem=s3.at[chunk, 2],
            recv_sem=r3.at[chunk, 2],
            device_id=diagonal(step),
            device_id_type=MESH,
        )

    def from_below(chunk):
        ring(chunk, 0, 3, 1).wait_recv()
        if chunk < 2:
            ring(chunk, 2, 3, 1).start()
            pass_on(chunk, 3, 1).start()
        across(chunk, 3, core).start()

    def from_above(chunk):
        ring(chunk, 1, 1, 3).wait_recv()
        if chunk >= 2:
            ring(chunk, 2, 1, 3).start()
            pass_on(chunk, 1, 3).start()
        across(chunk, 1, core).start()

    def from_far(chunk):
        ring(chunk, 2, 2, 1).wait_recv()

    for up, down in ((0, 2), (1, 3), (2, 0), (3, 1)):
        ring(up, 0, 0, 1).start()
        ring(down, 1, 0, 3).start()
    for chunk in range(4):
        across(chunk, 0, core).start()

    transpose_slabs(6, 12)

    def from_other(slot):
        for chunk in range(4):
            across(chunk, slot, 1 - core).wait_recv()

    def lines(slot, buf):
        line_y = (y + slot) % 4
        ty_all = ty[...]
        for kg in range(2):
            d0, d1 = band[kg, line_y, 0], band[kg, line_y, 1]
            real = jnp.concatenate([d0[:256], d1[:256]], axis=1)
            imag = jnp.concatenate([d0[256:], d1[256:]], axis=1)
            top = jnp.concatenate([real, imag], axis=1)
            low_half = jnp.concatenate([imag, -real], axis=1)
            data = jnp.concatenate([top, low_half], axis=0)
            data = lax.dot_general(data, mix[...], NN, preferred_element_type=F32).astype(BF16)
            line = lax.dot_general(ty_all, data, NN, preferred_element_type=F32)
            for k in range(4):
                for s in range(16):
                    col[buf, s, pl.ds(kg * 4 + k, 32, stride=8), :] = line[
                        s * 32 : (s + 1) * 32, k * 128 : (k + 1) * 128
                    ]

    def loop(work, first, last, unroll):
        def body(i, _):
            for u in range(unroll):
                work(first + i * unroll + u)
            return 0

        lax.fori_loop(0, (last - first) // unroll, body, 0)

    def turned(t):
        t = swap(t)
        return jnp.where(low, t, -t)

    def window_part(s, bufs, lanes):
        lines_of = [col[b, s] for b in bufs]
        table = twin[s, :, lanes]
        parts = []
        for form in (lambda t: t, turned):
            source = jnp.concatenate([form(t) for t in lines_of], axis=1).astype(BF16)
            parts.append(lax.dot_general(table, source, NT, preferred_element_type=F32))
        return parts

    def own_window(s):
        real, imag = window_part(s, (0,), slice(0, 128))
        acc[s, 0:256] = real
        acc[s, 256:512] = imag

    def near_window(s):
        real, imag = window_part(s, (1, 2), slice(128, 384))
        acc[s, 0:256] += real
        acc[s, 256:512] += imag

    def to_window(s, win):
        real, imag = window_part(s, (0,), slice(384, 512))
        win[0:256] = (acc[s, 0:256] + real).astype(BF16)
        win[256:512] = (acc[s, 256:512] + imag).astype(BF16)

    def to_samples(s, win):
        for j in range(6):
            rows = cw[s, j * 256 : (j + 1) * 256, :]
            part = lax.dot_general(win[...], rows, NT, preferred_element_type=F32)
            gain = xwt[s, j].astype(F32)
            here = slice(j * 256, (j + 1) * 256)
            out[s, 0:1, here] = jnp.sum(part[:256] * gain, axis=0, keepdims=True)
            out[s, 1:2, here] = jnp.sum(part[256:] * gain, axis=0, keepdims=True)

    from_other(0)
    lines(0, 0)
    from_below(0)
    from_above(2)
    transpose_slabs(12, 16)
    from_below(1)
    from_above(3)
    loop(own_window, 0, 16, 4)
    from_below(2)
    from_above(0)
    from_below(3)
    from_above(1)
    from_other(3)
    lines(3, 2)
    from_other(1)
    lines(1, 1)
    loop(near_window, 0, 16, 4)

    def got_cw(s, _):
        cw_copy(s).wait()
        return 0

    lax.fori_loop(0, 16, got_cw, 0)
    from_far(0)
    from_far(2)
    from_far(1)
    from_far(3)
    from_other(2)
    lines(2, 0)
    to_window(0, win_a)
    wins = (win_a, win_b)

    for s in range(16):
        if s < 15:
            to_window(s + 1, wins[(s + 1) % 2])
        to_samples(s, wins[s % 2])

    def sent(i, _):
        piece((me + i) % 16, me).wait_send()
        return 0

    lax.fori_loop(1, 16, sent, 0)
    for chunk in range(4):
        ring(chunk, 0, 0, 1).wait_send()
        ring(chunk, 1, 0, 3).wait_send()
        ring(chunk, 2, 3, 1).wait_send()
        for slot in range(4):
            across(chunk, slot, core).wait_send()


def per_device(image, deapodization, offsets, cross_weight, x_weight):
    tz, ty, tx = (jnp.asarray(t) for t in tables())
    any_space = pl.BlockSpec(memory_space=pl.ANY)
    smem = pl.BlockSpec(memory_space=pltpu.SMEM)
    vmem = pl.BlockSpec(memory_space=pltpu.VMEM)
    dma = pltpu.SemaphoreType.DMA
    samples = pl.pallas_call(
        kernel,
        out_shape=jax.ShapeDtypeStruct((16, 2, 1536), F32),
        in_specs=[any_space, vmem, smem, smem] + [any_space] * 5,
        out_specs=vmem,
        scratch_shapes=[
            pltpu.VMEM((2, 16, 32, 256), BF16),
            pltpu.VMEM((2, 256, 128), BF16),
            pltpu.VMEM((512, 512), BF16),
            pltpu.VMEM((2, 256, 256), F32),
            pltpu.VMEM((32, 256), F32),
            pltpu.VMEM((8, 2, 32, 128), BF16),
            pltpu.VMEM((2, 2, 256, 128), BF16),
            pltpu.VMEM((2, 4, 2, 512, 128), BF16),
            pltpu.VMEM((512, 512), BF16),
            pltpu.VMEM((2, 256, 512), F32),
            pltpu.VMEM((16, 256, 512), BF16),
            pltpu.VMEM((16, 512, 256), F32),
            pltpu.VMEM((3, 16, 256, 128), F32),
            pltpu.VMEM((16, 1536, 256), BF16),
            pltpu.VMEM((8, 1536, 256), BF16),
            pltpu.VMEM((16, 6, 256, 256), BF16),
            pltpu.VMEM((512, 256), BF16),
            pltpu.VMEM((512, 256), BF16),
            dma((4,)),
            dma((16,)),
            dma((16,)),
            dma((16,)),
            dma((16,)),
            dma((4, 3)),
            dma((4, 3)),
            dma((4, 4)),
            dma((4, 4)),
        ],
        compiler_params=pltpu.CompilerParams(
            collective_id=0, has_side_effects=True, vmem_limit_bytes=67043328
        ),
        cost_estimate=pl.CostEstimate(flops=11_000_000_000, bytes_accessed=28_000_000, transcendentals=0),
        name="spokes",
    )(image, deapodization, deapodization, offsets, cross_weight[0], x_weight[0], tz, ty, tx)
    return samples[None]


def solution(mesh):
    return jax.shard_map(
        per_device,
        mesh=mesh,
        in_specs=(
            P(None, "wide", "narrow", None),
            P(),
            P(("wide", "narrow"), None),
            P(("wide", "narrow"), None, None, None),
            P(("wide", "narrow"), None, None, None),
        ),
        out_specs=P(("wide", "narrow"), None, None, None),
        check_vma=False,
    )
```
